32 devices in a mesh: gx: 8 (over y, x, core), gy: 4 (over z).
Axes of the slice: x: 2, y: 2, z: 4, core: 2. Of those that a mesh axis runs over, the one named last changes fastest.
Arguments:
- hidden: bfloat16 [256, 16384], P('gx', 'gy'), may hold values from -40 to 40
- lm_head: bfloat16 [16384, 65536], P('gy', 'gx'), may hold values from -1 to 1
- parent: int32 [256], replicated, may hold values from 0 to 255, as said below
- draft_token: int32 [256], replicated, may hold values from 0 to 65535
- draft_prob: float32 [256], replicated, may hold values from 0.01 to 1
- uniforms: float32 [256], replicated, may hold values from 0.01 to 1
- node_count: int32 [4], replicated, may hold values from 1 to 64, as said below
- accepted_end: int32 [4], replicated, may hold values from 0 to 63, as said below
Outputs:
- vertex_accept_slack: float32 [256], P('gx')
- lineage_least_slack: float32 [256], P('gx')
- extra_draw_score: float32 [4, 65536], P(None, 'gx')
The draws below stay inside these ranges and needn't reach their ends.
Inputs may be any that keep to these rules, and one draw needn't show every extreme that they name: A node's parent lies in the same sequence at a lower slot; slot 0 of each sequence is its own parent. `node_count`: some sequence has all 64 slots live. `accepted_end`: the slot of a live node of that sequence.
All inputs are finite; a program needn't handle non-finite values.
Results may differ from the reference program's by a relative error of at most 0.0003.
Values may be sent and summed in bfloat16 or wider, within the bound.
No kernel may reach another device: no remote copies, remote signals or barrier semaphores. Data moves between devices by JAX's collectives and lax.ppermute only.
A program may use at most 128 MiB of HBM per device.

```python
import math
import jax
import jax.numpy as jnp

D = 16384
VOCAB = 65536
TREE = 64
NODES = 256
SEQS = 4


def draw_hidden(key, part):
    scale_key = jax.random.fold_in(key, 11)
    value_key = jax.random.fold_in(key, 12)
    base = jnp.clip(jax.random.normal(value_key, (NODES, D), jnp.float32), -6.0, 6.0)
    scales = jnp.exp(jax.random.uniform(scale_key, (NODES, 1), jnp.float32, jnp.log(0.5), jnp.log(5.0)))
    values = base * scales
    return values.astype(jnp.bfloat16)


def draw_lm_head(key, part):
    scale_key = jax.random.fold_in(key, 21)
    value_key = jax.random.fold_in(key, 22)
    col_scales = jnp.exp(jax.random.uniform(scale_key, (1, VOCAB), jnp.float32, jnp.log(0.3), jnp.log(3.0)))
    spread = 3.0 / D ** 0.5
    base = jnp.clip(jax.random.normal(value_key, (D, VOCAB), jnp.float32), -6.0, 6.0)
    values = base * spread * col_scales
    return values.astype(jnp.bfloat16)


def draw_parent(key, part):
    node_index = jnp.arange(NODES, dtype=jnp.int32)
    local_index = node_index % TREE
    lowest = jnp.maximum(local_index - 4, 0)
    highest = jnp.maximum(local_index, 1)
    chosen = jax.random.randint(jax.random.fold_in(key, 31), (NODES,), lowest, highest)
    chosen = jnp.where(local_index == 0, 0, chosen)
    return (node_index - local_index + chosen).astype(jnp.int32)


def counts_and_ends(key):
    base_key = jax.random.fold_in(key, 41)
    counts = jax.random.randint(jax.random.fold_in(base_key, 1), (SEQS,), 1, TREE + 1)
    full_seq = jax.random.randint(jax.random.fold_in(base_key, 2), (), 0, SEQS)
    counts = counts.at[full_seq].set(TREE)
    end_slots = jax.random.randint(jax.random.fold_in(base_key, 3), (SEQS,), 0, counts)
    end_slots = end_slots.at[full_seq].set(TREE - 1)
    end_slots = end_slots.at[(full_seq + 1) % SEQS].set(0)
    return (counts.astype(jnp.int32), end_slots.astype(jnp.int32))


def draw_node_count(key, part):
    return counts_and_ends(key)[0]


def draw_accepted_end(key, part):
    return counts_and_ends(key)[1]


def plant(values, rng, least, top_value):
    longest = values.shape.index(max(values.shape))
    spots = []
    for shift in (0, 1):
        where = [jax.random.randint(jax.random.fold_in(rng, axis), (), 0, length) for axis, length in enumerate(values.shape)]
        where[longest] = (where[longest] + shift) % values.shape[longest]
        spots.append(tuple(where))
    return values.at[spots[0]].set(least).at[spots[1]].set(top_value)


def setup_inputs(seed: int = 0) -> dict:
    splits = jax.random.split(jax.random.key(seed), 9)
    hidden = draw_hidden(jax.random.fold_in(splits[8], 71), 0)
    lm_head = draw_lm_head(jax.random.fold_in(splits[8], 71), 0)
    parent = draw_parent(jax.random.fold_in(splits[8], 71), 0)
    draft_token = plant(jax.random.randint(splits[3], (NODES,), 0, VOCAB), jax.random.fold_in(splits[3], 1), 0, VOCAB - 1).astype(jnp.int32)
    draft_prob = jnp.clip(jnp.exp(jax.random.uniform(splits[4], (NODES,), jnp.float32, math.log(0.01), math.log(1.0))), 0.01, 1.0)
    uniforms = jnp.clip(jax.random.uniform(splits[5], (NODES,), jnp.float32, 0.01, 1.0), 0.01, 1.0)
    node_count = draw_node_count(jax.random.fold_in(splits[8], 71), 0)
    accepted_end = draw_accepted_end(jax.random.fold_in(splits[8], 71), 0)
    return {"hidden": hidden, "lm_head": lm_head, "parent": parent, "draft_token": draft_token, "draft_prob": draft_prob, "uniforms": uniforms, "node_count": node_count, "accepted_end": accepted_end}


big_margin = 10000.0


def reference(hidden, lm_head, parent, draft_token, draft_prob, uniforms, node_count, accepted_end):
    emitted_scores = jnp.dot(hidden, lm_head, preferred_element_type=jnp.float32)
    row_max = jnp.max(emitted_scores, axis=1)
    partition_function = row_max + jnp.log(jnp.sum(jnp.exp(emitted_scores - row_max[:, None]), axis=1))
    target = emitted_scores[parent, draft_token]
    margin = target - partition_function[parent] - jnp.log(draft_prob) - jnp.log(uniforms)
    node_index = jnp.arange(NODES, dtype=jnp.int32)
    local_index = node_index % TREE
    live_mask = local_index < node_count[node_index // TREE]
    root_mask = parent == node_index
    spare_mask = jnp.logical_or(root_mask, jnp.logical_not(live_mask))
    vertex_accept_slack = jnp.where(spare_mask, jnp.float32(0.0), margin)
    path_min = jnp.where(root_mask, jnp.float32(big_margin), margin)
    ancestor = parent
    for _ in range((TREE - 1).bit_length()):
        path_min = jnp.minimum(path_min, path_min[ancestor])
        ancestor = ancestor[ancestor]
    lineage_least_slack = jnp.where(spare_mask, jnp.float32(0.0), path_min)
    leaf_entries = jnp.arange(SEQS, dtype=jnp.int32) * TREE + accepted_end
    extra_draw_score = emitted_scores[leaf_entries] - partition_function[leaf_entries][:, None]
    return vertex_accept_slack, lineage_least_slack, extra_draw_score
```

```python
import functools

import jax
import jax.numpy as jnp
from jax import lax
from jax.experimental import pallas as pl
from jax.experimental.pallas import tpu as pltpu
from jax.sharding import PartitionSpec as P


big_margin = 10000.0
f32 = jnp.float32
bf16 = jnp.bfloat16
i32 = jnp.int32
i16 = jnp.int16
STEPS = 256.0
LEVELS = 32760.0
VMEM_LIMIT = 56 * 1024 * 1024


def iota(shape, dim):
    return lax.broadcasted_iota(i32, shape, dim)


def to_row(mask, col):
    return jnp.sum(jnp.where(mask, col, 0.0), axis=0, keepdims=True)


def to_col(mask, row):
    return jnp.sum(jnp.where(mask, row, 0.0), axis=1, keepdims=True)


def whole(shape):
    return pl.BlockSpec(shape, lambda *_: (0,) * len(shape))


def prep_kernel(place, counts, ends, parent_row, token, sel, reach, prow, picks, branch, *, seqs, block, xor, limits, spans):
    nodes = parent_row.shape[1]
    tree = nodes // seqs
    square = (nodes, nodes)
    up, side = iota(square, 0), iota(square, 1)
    prow_in = parent_row[...]
    pcol_in = to_col(up == side, prow_in.astype(f32)).astype(i32)

    def flags(index, parents):
        live = index < 0
        end = jnp.full(index.shape, -1, i32)
        for s in range(seqs):
            inside = (index >= s * tree) & (index < (s + 1) * tree)
            live = live | (inside & (index - s * tree < counts[s]))
            end = jnp.where(index == s * tree + ends[s], s, end)
        want = jnp.where(live & (parents != index), 1.0, 0.0).astype(f32)
        return want, end

    row_i, col_i = iota((1, nodes), 1), iota((nodes, 1), 0)
    want_row, end_row = flags(row_i, prow_in)
    want_col, end_col = flags(col_i, pcol_in)
    need_col = jnp.max(jnp.where(prow_in == up, want_row, 0.0), axis=1, keepdims=True)
    need_row = jnp.max(jnp.where(pcol_in == side, want_col, 0.0), axis=0, keepdims=True)
    other_col = jnp.where(end_col >= 0, 0.0, need_col)
    other_row = jnp.where(end_row >= 0, 0.0, need_row)
    before = to_col(side < up, other_row) + seqs
    pos_col = jnp.where(end_col >= 0, end_col.astype(f32), jnp.where(other_col > 0, before, -1.0))
    parent_pos = to_row(up == prow_in, pos_col).astype(i32)
    prow[...] = parent_pos
    total = jnp.sum(other_row, axis=1, keepdims=True) + seqs
    choice = jnp.zeros((1, 1), f32)
    for limit in limits:
        choice = choice + jnp.where(total > limit, 1.0, 0.0)
    branch[...] = jnp.broadcast_to(choice, branch.shape).astype(i32)
    width, quarter = spans
    column = token[...] - (place[0] * width + place[1] * quarter)
    inside = (column >= 0) & (column < quarter) & (parent_pos >= 0)
    safe = jnp.clip(column, 0, quarter - 1)
    row = jnp.maximum(parent_pos, 0)
    picks[0:1, :] = jnp.where(inside, row // 8 * 8, 0)
    picks[1:2, :] = jnp.where(inside, safe // 128 * 128, 0)
    picks[2:3, :] = jnp.where(inside, row % 8 * 128 + safe % 128, -1)
    if xor:
        origin = (lax.bitwise_xor(row_i // block, place[0])) * block + row_i % block
    else:
        origin = row_i
    pos_x = to_row(up == origin, pos_col)
    sel[...] = jnp.where(pos_x == iota(sel.shape, 0).astype(f32), 1.0, 0.0).astype(bf16)
    chain = jnp.where((pcol_in == side) | (up == side), 1.0, 0.0).astype(bf16)
    for _ in range((tree - 1).bit_length()):
        chain = jnp.minimum(jnp.dot(chain, chain, preferred_element_type=f32), 1.0).astype(bf16)
    reach[...] = chain


def prep(place, counts, ends, parent, token, seqs, block, xor, padded, limits, spans):
    nodes = parent.shape[0]
    smem = pl.BlockSpec(memory_space=pltpu.SMEM)
    return pl.pallas_call(
        functools.partial(
            prep_kernel, seqs=seqs, block=block, xor=xor, limits=limits, spans=spans
        ),
        in_specs=[smem, smem, smem, whole((1, nodes)), whole((1, nodes))],
        out_specs=[whole((padded, nodes)), whole((nodes, nodes)), whole((1, nodes)), whole((3, nodes)), whole((1, 128))],
        out_shape=[
            jax.ShapeDtypeStruct((padded, nodes), bf16),
            jax.ShapeDtypeStruct((nodes, nodes), bf16),
            jax.ShapeDtypeStruct((1, nodes), i32),
            jax.ShapeDtypeStruct((3, nodes), i32),
            jax.ShapeDtypeStruct((1, 128), i32),
        ],
        grid=(1,),
        compiler_params=pltpu.CompilerParams(vmem_limit_bytes=VMEM_LIMIT),
        cost_estimate=pl.CostEstimate(flops=4 * 10**9, bytes_accessed=4 * nodes * nodes, transcendentals=0),
        name="prep",
    )(place, counts, ends, parent.reshape(1, nodes), token.reshape(1, nodes))


def lanes_for(rows, width):
    return min(width, pl.cdiv(rows, 128) * 128)


def encode(value, out):
    rows, width = value.shape
    top = jnp.maximum(jnp.max(jnp.abs(value), axis=1, keepdims=True), 1e-20)
    code = jnp.ceil(jnp.log(top) * (STEPS / jnp.log(2.0).astype(f32)))
    inverse = LEVELS * jnp.exp2(code * (-1.0 / STEPS))
    coded = jnp.round(value * inverse)
    out[...] = coded.astype(i32).astype(i16)
    lanes = lanes_for(rows, width)
    spare = pl.cdiv(rows, lanes)
    tail = coded[rows - 16 : rows, 0:lanes]
    slot = iota((16, 1), 0)
    for i in range(spare):
        match = iota((rows, lanes), 0) == iota((rows, lanes), 1) + i * lanes
        tail = jnp.where(slot == 16 - spare + i, to_row(match, code), tail)
    out[rows - 16 : rows, 0:lanes] = tail.astype(i32).astype(i16)


def decode(ref):
    rows, width = ref.shape
    lanes = lanes_for(rows, width)
    spare = pl.cdiv(rows, lanes)
    tail = ref[rows - 16 : rows, 0:lanes].astype(i32).astype(f32)
    code = jnp.zeros((rows, 1), f32)
    for i in range(spare):
        match = iota((rows, lanes), 0) == iota((rows, lanes), 1) + i * lanes
        code = code + to_col(match, tail[16 - spare + i : 17 - spare + i, :])
    scale = jnp.exp2(code * (1.0 / STEPS)) * (1.0 / LEVELS)
    return ref[...].astype(i32).astype(f32) * scale


def ring_kernel(z, *refs, blocks, halves, parties, arrivals, ordered):
    refs = list(refs)
    first, own = blocks > 0, arrivals < 0
    if first:
        sel = refs.pop(0)
        parts = [refs.pop(0) for _ in range(blocks)]
    else:
        lhs = refs.pop(0)
    weights = refs.pop(0)
    received = [refs.pop(0) for _ in range(max(arrivals, 0))]
    if ordered:
        refs.pop(0)
    if first:
        lhs = refs.pop(0)
    outs = [refs.pop(0) for _ in range(1 if own else 2)]
    buffer, acc, ready = refs[:3]
    tiles, td, h = buffer.shape
    quarter = weights.shape[1] // parties
    per = tiles // 2
    starts = [
        lax.rem(z[0] + parties + distance, parties) * quarter + side * h for distance, side in halves
    ]

    def fetch(tile):
        column = pl.multiple_of(jnp.where(tile < per, starts[0], starts[1]), h)
        depth = pl.multiple_of(lax.rem(tile, per) * td, td)
        return pltpu.make_async_copy(
            weights.at[pl.ds(depth, td), pl.ds(column, h)], buffer.at[tile], ready.at[tile]
        )

    ahead = min(tiles, 4)
    for tile in range(ahead):
        fetch(tile).start()
    if first:
        stacked = refs[3]
        height = parts[0].shape[0]
        for j, part in enumerate(parts):
            stacked[j * height : (j + 1) * height, :] = part[...]
        span = min(512, stacked.shape[1])

        def compact(j, carry):
            column = pl.ds(pl.multiple_of(j * span, span), span)
            lhs[:, column] = jnp.dot(
                sel[...], stacked[:, column], preferred_element_type=f32
            ).astype(bf16)
            return carry

        lax.fori_loop(0, stacked.shape[1] // span, compact, 0)

    def finish_half(i):
        if own:
            outs[0][:, i * h : (i + 1) * h] = acc[...]
            return
        value = acc[...]
        if arrivals:
            value = value + decode(received[i])
        encode(value, outs[i])

    def step(tile, carry):
        @pl.when(tile + ahead < tiles)
        def _():
            fetch(tile + ahead).start()

        fetch(tile).wait()
        j = lax.rem(tile, per)
        depth = pl.multiple_of(j * td, td)
        value = jnp.dot(lhs[:, pl.ds(depth, td)], buffer[tile], preferred_element_type=f32)
        acc[...] = value + jnp.where(j == 0, 0.0, acc[...])
        for i in range(2):
            pl.when(tile == (i + 1) * per - 1)(functools.partial(finish_half, i))
        return carry

    acc[...] = jnp.zeros(acc.shape, f32)
    lax.fori_loop(0, tiles, step, 0)


def ring_product(z, lhs, weights, rows, halves, parties, received, own, after):
    depth, width = weights.shape
    h = width // parties // 2
    td = depth // 4
    anywhere = pl.BlockSpec(memory_space=pl.ANY)
    out_shape, out_specs, extra = [], [], []
    first = isinstance(lhs, tuple)
    blocks = 0
    if first:
        sel, parts = lhs
        nodes = sel.shape[1]
        blocks = len(parts)
        args = [sel, *parts]
        in_specs = [whole((rows, nodes))] + [whole(part.shape) for part in parts]
        out_shape.append(jax.ShapeDtypeStruct((rows, depth), bf16))
        out_specs.append(whole((rows, depth)))
        extra.append(pltpu.VMEM((nodes, depth), bf16))
    else:
        args, in_specs = [lhs], [whole((rows, depth))]
    args.append(weights)
    in_specs.append(anywhere)
    args.extend(received)
    in_specs.extend(whole(a.shape) for a in received)
    if after is not None:
        args.append(after)
        in_specs.append(anywhere)
    if own:
        out_shape.append(jax.ShapeDtypeStruct((rows, 2 * h), f32))
        out_specs.append(whole((rows, 2 * h)))
    else:
        out_shape.extend([jax.ShapeDtypeStruct((rows, h), i16)] * 2)
        out_specs.extend([whole((rows, h))] * 2)
    return pl.pallas_call(
        functools.partial(
            ring_kernel,
            blocks=blocks,
            halves=halves,
            parties=parties,
            arrivals=-1 if own else len(received),
            ordered=after is not None,
        ),
        grid_spec=pltpu.PrefetchScalarGridSpec(
            num_scalar_prefetch=1,
            grid=(1,),
            in_specs=in_specs,
            out_specs=out_specs,
            scratch_shapes=[
                pltpu.VMEM((8, td, h), bf16),
                pltpu.VMEM((rows, h), f32),
                pltpu.SemaphoreType.DMA((8,)),
            ]
            + extra,
        ),
        out_shape=out_shape,
        compiler_params=pltpu.CompilerParams(vmem_limit_bytes=36 * 2**20),
        cost_estimate=pl.CostEstimate(
            flops=4 * depth * width * rows // parties + 4 * 10**9,
            bytes_accessed=2 * depth * width // parties,
            transcendentals=0,
        ),
        name=f"ring_{rows}",
    )(z, *args)


def settle_kernel(picks, own, *refs):
    refs = list(refs)
    payload, logits, picked = refs[-3:]
    pairs = refs[:-3]
    rows, width = own.shape
    h = width // 2
    nodes = picked.shape[0] // 8
    seqs = payload.shape[0] - 2 * stat_height(nodes, width)
    halves = [own[:, 0:h], own[:, h:width]]
    for group in range(len(pairs) // 2):
        forward, backward = decode(pairs[2 * group]), decode(pairs[2 * group + 1])
        if group == 0:
            halves = [halves[0] + forward, halves[1] + backward]
        else:
            halves = [halves[0] + backward, halves[1] + forward]
    top = jnp.maximum(*[jnp.max(half, axis=1, keepdims=True) for half in halves])
    total = jnp.zeros((rows, 1), f32)
    for i, half in enumerate(halves):
        logits[:, i * h : (i + 1) * h] = half
        total = total + jnp.sum(jnp.exp(half - top), axis=1, keepdims=True)
    lse = top + jnp.log(total)
    payload[...] = jnp.zeros(payload.shape, f32)
    payload[0:seqs, :] = logits[0:seqs, :]
    flat = iota((8, 128), 0) * 128 + iota((8, 128), 1)

    def pick(group, carry):
        for j in range(8):
            n = group * 8 + j
            base = pl.multiple_of(jnp.minimum(picks[0, n], rows - 8), 8)
            start = pl.multiple_of(picks[1, n], 128)
            tile = logits[pl.ds(base, 8), pl.ds(start, 128)]
            picked[pl.ds(pl.multiple_of(n * 8, 8), 8), :] = jnp.where(flat == picks[2, n], tile, 0.0)
        return carry

    lax.fori_loop(0, nodes // 8, pick, 0)
    target = jnp.sum(jnp.sum(picked[...].reshape(nodes, 8, 128), axis=1), axis=1, keepdims=True)
    lanes = min(width, nodes)
    stat_rows = stat_height(nodes, width)
    for i in range(stat_rows):
        match = iota((rows, lanes), 0) == iota((rows, lanes), 1) + i * lanes
        payload[seqs + i : seqs + i + 1, 0:lanes] = to_row(match, lse)
        match = iota((nodes, lanes), 0) == iota((nodes, lanes), 1) + i * lanes
        at = seqs + stat_rows + i
        payload[at : at + 1, 0:lanes] = to_row(match, target)


def stat_height(nodes, width):
    return pl.cdiv(nodes, width)


def settle(picks, own, pairs, seqs):
    rows, width = own.shape
    nodes = picks.shape[1]
    height = seqs + 2 * stat_height(nodes, width)
    return pl.pallas_call(
        settle_kernel,
        grid_spec=pltpu.PrefetchScalarGridSpec(
            num_scalar_prefetch=1,
            grid=(1,),
            in_specs=[whole(a.shape) for a in (own, *pairs)],
            out_specs=whole((height, width)),
            scratch_shapes=[pltpu.VMEM((rows, width), f32), pltpu.VMEM((nodes * 8, 128), f32)],
        ),
        out_shape=jax.ShapeDtypeStruct((height, width), f32),
        compiler_params=pltpu.CompilerParams(vmem_limit_bytes=36 * 2**20),
        name=f"settle_{rows}",
    )(picks, own, *pairs)


def combine_kernel(*refs, seqs):
    stats = refs[-1]
    parts = refs[:-1]
    nodes, width = stats.shape[1], parts[0].shape[1]
    lanes = min(nodes, width)
    stat_rows = stat_height(nodes, width)
    for i in range(stat_rows):
        values = [ref[seqs + i : seqs + i + 1, 0:lanes] for ref in parts]
        top = functools.reduce(jnp.maximum, values)
        total = sum(jnp.exp(value - top) for value in values)
        stats[0:1, i * lanes : (i + 1) * lanes] = top + jnp.log(total)
        at = seqs + stat_rows + i
        stats[1:2, i * lanes : (i + 1) * lanes] = sum(ref[at : at + 1, 0:lanes] for ref in parts)


def combine(payloads, nodes, seqs):
    return pl.pallas_call(
        functools.partial(combine_kernel, seqs=seqs),
        grid=(1,),
        in_specs=[whole(a.shape) for a in payloads],
        out_specs=whole((2, nodes)),
        out_shape=jax.ShapeDtypeStruct((2, nodes), f32),
        compiler_params=pltpu.CompilerParams(vmem_limit_bytes=16 * 2**20),
        name="combine",
    )(*payloads)


def finish_kernel(place, counts, stats, *refs, parties, seqs):
    refs = list(refs)
    leaves = [refs.pop(0) for _ in range(parties)]
    prow, parent, prob, uniform, reach, vertex, lineage, score = refs
    nodes = prow.shape[1]
    tree = nodes // seqs
    out_rows = vertex.shape[1]
    top = jnp.max(stats[:, 0, :], axis=0, keepdims=True)
    total = jnp.sum(jnp.exp(stats[:, 0, :] - top), axis=0, keepdims=True)
    target = jnp.sum(stats[:, 1, :], axis=0, keepdims=True)
    square = (nodes, nodes)
    up, side = iota(square, 0), iota(square, 1)
    log_total = to_col(up == side, top + jnp.log(total))
    width = leaves[0].shape[1]
    for j, ref in enumerate(leaves):
        owner = (place[1] + parties - j) % parties
        score[:, pl.ds(pl.multiple_of(owner * width, width), width)] = ref[0:seqs, :] - log_total[0:seqs, :]
    margin = target - to_row(up == prow[...], log_total) - jnp.log(prob[...]) - jnp.log(uniform[...])
    index = iota((1, nodes), 1)
    root = parent[...] == index
    live = index < 0
    for s in range(seqs):
        inside = (index >= s * tree) & (index < (s + 1) * tree)
        live = live | (inside & (index - s * tree < counts[s]))
    keep = jnp.logical_not(root) & live
    bounded = jnp.where(root, big_margin, margin)
    path = jnp.min(jnp.where(reach[...].astype(f32) > 0, bounded, big_margin), axis=1, keepdims=True)
    kept = to_col(up == side, jnp.where(keep, 1.0, 0.0))
    vertex_col = to_col(up == side, jnp.where(keep, margin, 0.0))
    local = iota((nodes, out_rows), 0) == iota((nodes, out_rows), 1) + place[0] * out_rows
    vertex[...] = to_row(local, vertex_col)
    lineage[...] = to_row(local, jnp.where(kept > 0, path, 0.0))


def finish(place, counts, stats, leaves, prow, parent, prob, uniform, reach, out_rows):
    parties = len(leaves)
    nodes = prow.shape[1]
    seqs, width = counts.shape[0], leaves[0].shape[1]
    smem = pl.BlockSpec(memory_space=pltpu.SMEM)
    rows = [prow, parent.reshape(1, nodes), prob.reshape(1, nodes), uniform.reshape(1, nodes)]
    arrays = [stats, *leaves, *rows, reach]
    return pl.pallas_call(
        functools.partial(finish_kernel, parties=parties, seqs=seqs),
        grid=(1,),
        in_specs=[smem, smem] + [whole(a.shape) for a in arrays],
        out_specs=[whole((1, out_rows)), whole((1, out_rows)), whole((seqs, width * parties))],
        out_shape=[
            jax.ShapeDtypeStruct((1, out_rows), f32),
            jax.ShapeDtypeStruct((1, out_rows), f32),
            jax.ShapeDtypeStruct((seqs, width * parties), f32),
        ],
        compiler_params=pltpu.CompilerParams(vmem_limit_bytes=VMEM_LIMIT),
        name="finish",
    )(place, counts, *arrays)


def gathered(hidden, marker):
    size = lax.axis_size("gx")
    if size != 8:
        return [lax.all_gather(hidden, "gx", axis=0, tiled=True)]

    def swap(value, k):
        return lax.ppermute(value, "gx", [(i, i ^ k) for i in range(size)])

    parts = [None] * size
    parts[0] = hidden
    parts[1] = swap(hidden, 1)
    for k in (6, 2, 4):
        parts[k] = swap(hidden, k)
    for k in (2, 4, 6):
        passed, marker = lax.optimization_barrier((parts[k], marker))
        parts[k + 1] = swap(passed, 1)
    return parts


def bucket_sizes(nodes, h):
    sizes = []
    for k in (6, 7, 8, 9, 11):
        sizes.append(nodes * k // 16)
    largest = nodes
    while largest - pl.cdiv(largest, lanes_for(largest, h)) < nodes:
        largest += 16
    return sizes + [largest]


def local(hidden, lm_head, parent, draft_token, draft_prob, uniforms, node_count, accepted_end):
    nodes = parent.shape[0]
    seqs = node_count.shape[0]
    out_rows = hidden.shape[0]
    parties = lax.axis_size("gy")
    h = lm_head.shape[1] // parties // 2
    gx, gy = lax.axis_index("gx").astype(i32), lax.axis_index("gy").astype(i32)
    place = jnp.concatenate([gx.reshape(1), gy.reshape(1)])
    sizes = bucket_sizes(nodes, h)
    sel, reach, prow, picks, branch = prep(
        place,
        node_count,
        accepted_end,
        parent,
        draft_token,
        seqs,
        out_rows,
        lax.axis_size("gx") == 8,
        sizes[-1],
        [size - pl.cdiv(size, lanes_for(size, h)) for size in sizes[:-1]],
        (lm_head.shape[1], lm_head.shape[1] // parties),
    )
    parts = gathered(hidden, branch)
    z = gy.reshape(1)

    def shift(value, k):
        return lax.ppermute(value, "gy", [(i, (i + k) % parties) for i in range(parties)])

    def run(rows):
        def body():
            state = {"lhs": (sel, parts), "after": None}

            def product(halves, received, own=False):
                out = ring_product(
                    z, state["lhs"], lm_head, rows, halves, parties, received, own, state["after"]
                )
                if isinstance(state["lhs"], tuple):
                    state["lhs"], out = out[0], out[1:]
                state["after"] = out[0]
                return out

            def exchange(out):
                return [shift(out[0], 1), shift(out[1], -1)]

            reach_out = parties // 2
            major = exchange(product(((reach_out, 0), (-reach_out, 1)), []))
            minor = []
            for d in range(reach_out - 1, 0, -1):
                minor = exchange(product(((d, 1), (-d, 0)), minor))
                major = exchange(product(((d, 0), (-d, 1)), major))
            own = product(((0, 0), (0, 1)), [], own=True)
            return settle(picks, own[0], [*major, *minor], seqs)

        return body

    payload = lax.switch(branch[0, 0], [run(size) for size in sizes])
    payloads = [payload] + [shift(payload, k) for k in range(1, parties)]
    stats = lax.all_gather(combine(payloads, nodes, seqs), "gx")
    vertex, lineage, score = finish(
        place, node_count, stats, payloads, prow, parent, draft_prob, uniforms, reach, out_rows
    )
    return vertex.reshape(out_rows), lineage.reshape(out_rows), score


def solution(mesh):
    return jax.shard_map(
        local,
        mesh=mesh,
        in_specs=(P("gx", "gy"), P("gy", "gx"), P(), P(), P(), P(), P(), P()),
        out_specs=(P("gx"), P("gx"), P(None, "gx")),
        check_vma=False,
    )
```

```python
import functools

import jax
import jax.numpy as jnp
from jax import lax
from jax.experimental import pallas as pl
from jax.experimental.pallas import tpu as pltpu
from jax.sharding import PartitionSpec as P


big_margin = 10000.0
f32 = jnp.float32
bf16 = jnp.bfloat16
i32 = jnp.int32
i16 = jnp.int16
STEPS = 256.0
LEVELS = 32760.0
VMEM_LIMIT = 56 * 1024 * 1024


def iota(shape, dim):
    return lax.broadcasted_iota(i32, shape, dim)


def to_row(mask, col):
    return jnp.sum(jnp.where(mask, col, 0.0), axis=0, keepdims=True)


def to_col(mask, row):
    return jnp.sum(jnp.where(mask, row, 0.0), axis=1, keepdims=True)


def whole(shape):
    return pl.BlockSpec(shape, lambda *_: (0,) * len(shape))


def prep_kernel(place, counts, ends, parent_row, token, sel, reach, prow, picks, branch, *, seqs, block, xor, limits, spans):
    nodes = parent_row.shape[1]
    tree = nodes // seqs
    square = (nodes, nodes)
    up, side = iota(square, 0), iota(square, 1)
    prow_in = parent_row[...]
    pcol_in = to_col(up == side, prow_in.astype(f32)).astype(i32)

    def flags(index, parents):
        live = index < 0
        end = jnp.full(index.shape, -1, i32)
        for s in range(seqs):
            inside = (index >= s * tree) & (index < (s + 1) * tree)
            live = live | (inside & (index - s * tree < counts[s]))
            end = jnp.where(index == s * tree + ends[s], s, end)
        want = jnp.where(live & (parents != index), 1.0, 0.0).astype(f32)
        return want, end

    row_i, col_i = iota((1, nodes), 1), iota((nodes, 1), 0)
    want_row, end_row = flags(row_i, prow_in)
    want_col, end_col = flags(col_i, pcol_in)
    need_col = jnp.max(jnp.where(prow_in == up, want_row, 0.0), axis=1, keepdims=True)
    need_row = jnp.max(jnp.where(pcol_in == side, want_col, 0.0), axis=0, keepdims=True)
    other_col = jnp.where(end_col >= 0, 0.0, need_col)
    other_row = jnp.where(end_row >= 0, 0.0, need_row)
    before = to_col(side < up, other_row) + seqs
    pos_col = jnp.where(end_col >= 0, end_col.astype(f32), jnp.where(other_col > 0, before, -1.0))
    parent_pos = to_row(up == prow_in, pos_col).astype(i32)
    prow[...] = parent_pos
    total = jnp.sum(other_row, axis=1, keepdims=True) + seqs
    choice = jnp.zeros((1, 1), f32)
    for limit in limits:
        choice = choice + jnp.where(total > limit, 1.0, 0.0)
    branch[...] = jnp.broadcast_to(choice, branch.shape).astype(i32)
    width, quarter = spans
    column = token[...] - (place[0] * width + place[1] * quarter)
    inside = (column >= 0) & (column < quarter) & (parent_pos >= 0)
    safe = jnp.clip(column, 0, quarter - 1)
    row = jnp.maximum(parent_pos, 0)
    hit = jnp.where(inside, 1.0, 0.0)
    rank_col = jnp.where(to_col(up == side, hit) > 0, to_col(side < up, hit), -1.0)
    chosen = rank_col == side.astype(f32)
    fields = [row // 8 * 8, safe // 128 * 128, row % 8 * 128 + safe % 128, row_i]
    for i, field in enumerate(fields):
        picks[i : i + 1, :] = to_row(chosen, to_col(up == side, field.astype(f32))).astype(i32)
    found = jnp.sum(hit, axis=1, keepdims=True)
    picks[4:5, :] = jnp.broadcast_to(found, (1, nodes)).astype(i32)
    if xor:
        origin = (lax.bitwise_xor(row_i // block, place[0])) * block + row_i % block
    else:
        origin = row_i
    pos_x = to_row(up == origin, pos_col)
    sel[...] = jnp.where(pos_x == iota(sel.shape, 0).astype(f32), 1.0, 0.0).astype(bf16)
    chain = jnp.where((pcol_in == side) | (up == side), 1.0, 0.0).astype(bf16)
    for _ in range((tree - 1).bit_length()):
        chain = jnp.minimum(jnp.dot(chain, chain, preferred_element_type=f32), 1.0).astype(bf16)
    reach[...] = chain


def prep(place, counts, ends, parent, token, seqs, block, xor, padded, limits, spans):
    nodes = parent.shape[0]
    smem = pl.BlockSpec(memory_space=pltpu.SMEM)
    return pl.pallas_call(
        functools.partial(
            prep_kernel, seqs=seqs, block=block, xor=xor, limits=limits, spans=spans
        ),
        in_specs=[smem, smem, smem, whole((1, nodes)), whole((1, nodes))],
        out_specs=[whole((padded, nodes)), whole((nodes, nodes)), whole((1, nodes)), whole((5, nodes)), whole((1, 128))],
        out_shape=[
            jax.ShapeDtypeStruct((padded, nodes), bf16),
            jax.ShapeDtypeStruct((nodes, nodes), bf16),
            jax.ShapeDtypeStruct((1, nodes), i32),
            jax.ShapeDtypeStruct((5, nodes), i32),
            jax.ShapeDtypeStruct((1, 128), i32),
        ],
        grid=(1,),
        compiler_params=pltpu.CompilerParams(vmem_limit_bytes=VMEM_LIMIT),
        cost_estimate=pl.CostEstimate(flops=4 * 10**9, bytes_accessed=4 * nodes * nodes, transcendentals=0),
        name="prep",
    )(place, counts, ends, parent.reshape(1, nodes), token.reshape(1, nodes))


def lanes_for(rows, width):
    return min(width, pl.cdiv(rows, 128) * 128)


def encode(value, out):
    rows, width = value.shape
    top = jnp.maximum(jnp.max(jnp.abs(value), axis=1, keepdims=True), 1e-20)
    code = jnp.ceil(jnp.log(top) * (STEPS / jnp.log(2.0).astype(f32)))
    inverse = LEVELS * jnp.exp2(code * (-1.0 / STEPS))
    coded = jnp.round(value * inverse)
    out[...] = coded.astype(i32).astype(i16)
    lanes = lanes_for(rows, width)
    spare = pl.cdiv(rows, lanes)
    tail = coded[rows - 16 : rows, 0:lanes]
    slot = iota((16, 1), 0)
    for i in range(spare):
        match = iota((rows, lanes), 0) == iota((rows, lanes), 1) + i * lanes
        tail = jnp.where(slot == 16 - spare + i, to_row(match, code), tail)
    out[rows - 16 : rows, 0:lanes] = tail.astype(i32).astype(i16)


def decode(ref):
    rows, width = ref.shape
    lanes = lanes_for(rows, width)
    spare = pl.cdiv(rows, lanes)
    tail = ref[rows - 16 : rows, 0:lanes].astype(i32).astype(f32)
    code = jnp.zeros((rows, 1), f32)
    for i in range(spare):
        match = iota((rows, lanes), 0) == iota((rows, lanes), 1) + i * lanes
        code = code + to_col(match, tail[16 - spare + i : 17 - spare + i, :])
    scale = jnp.exp2(code * (1.0 / STEPS)) * (1.0 / LEVELS)
    return ref[...].astype(i32).astype(f32) * scale


def ring_kernel(z, *refs, blocks, halves, parties, arrivals, ordered):
    refs = list(refs)
    first, own = blocks > 0, arrivals < 0
    if first:
        sel = refs.pop(0)
        parts = [refs.pop(0) for _ in range(blocks)]
    else:
        lhs = refs.pop(0)
    weights = refs.pop(0)
    received = [refs.pop(0) for _ in range(max(arrivals, 0))]
    if ordered:
        refs.pop(0)
    if first:
        lhs = refs.pop(0)
    outs = [refs.pop(0) for _ in range(1 if own else 2)]
    buffer, acc, ready = refs[:3]
    tiles, td, h = buffer.shape
    quarter = weights.shape[1] // parties
    per = tiles // 2
    starts = [
        lax.rem(z[0] + parties + distance, parties) * quarter + side * h for distance, side in halves
    ]

    def fetch(tile):
        column = pl.multiple_of(jnp.where(tile < per, starts[0], starts[1]), h)
        depth = pl.multiple_of(lax.rem(tile, per) * td, td)
        return pltpu.make_async_copy(
            weights.at[pl.ds(depth, td), pl.ds(column, h)], buffer.at[tile], ready.at[tile]
        )

    for tile in range(tiles):
        fetch(tile).start()
    if first:
        stacked = refs[3]
        height = parts[0].shape[0]
        for j, part in enumerate(parts):
            stacked[j * height : (j + 1) * height, :] = part[...]
        span = min(512, stacked.shape[1])

        def compact(j, carry):
            column = pl.ds(pl.multiple_of(j * span, span), span)
            lhs[:, column] = jnp.dot(
                sel[...], stacked[:, column], preferred_element_type=f32
            ).astype(bf16)
            return carry

        lax.fori_loop(0, stacked.shape[1] // span, compact, 0)

    def finish_half(i):
        if own:
            outs[0][:, i * h : (i + 1) * h] = acc[...]
            return
        value = acc[...]
        if arrivals:
            value = value + decode(received[i])
        encode(value, outs[i])

    def step(tile, carry):
        fetch(tile).wait()
        j = lax.rem(tile, per)
        depth = pl.multiple_of(j * td, td)
        value = jnp.dot(lhs[:, pl.ds(depth, td)], buffer[tile], preferred_element_type=f32)
        acc[...] = value + jnp.where(j == 0, 0.0, acc[...])
        for i in range(2):
            pl.when(tile == (i + 1) * per - 1)(functools.partial(finish_half, i))
        return carry

    acc[...] = jnp.zeros(acc.shape, f32)
    lax.fori_loop(0, tiles, step, 0)


def ring_product(z, lhs, weights, rows, halves, parties, received, own, after):
    depth, width = weights.shape
    h = width // parties // 2
    td = depth // 4
    anywhere = pl.BlockSpec(memory_space=pl.ANY)
    out_shape, out_specs, extra = [], [], []
    first = isinstance(lhs, tuple)
    blocks = 0
    if first:
        sel, parts = lhs
        nodes = sel.shape[1]
        blocks = len(parts)
        args = [sel, *parts]
        in_specs = [whole((rows, nodes))] + [whole(part.shape) for part in parts]
        out_shape.append(jax.ShapeDtypeStruct((rows, depth), bf16))
        out_specs.append(whole((rows, depth)))
        extra.append(pltpu.VMEM((nodes, depth), bf16))
    else:
        args, in_specs = [lhs], [whole((rows, depth))]
    args.append(weights)
    in_specs.append(anywhere)
    args.extend(received)
    in_specs.extend(whole(a.shape) for a in received)
    if after is not None:
        args.append(after)
        in_specs.append(anywhere)
    if own:
        out_shape.append(jax.ShapeDtypeStruct((rows, 2 * h), f32))
        out_specs.append(whole((rows, 2 * h)))
    else:
        out_shape.extend([jax.ShapeDtypeStruct((rows, h), i16)] * 2)
        out_specs.extend([whole((rows, h))] * 2)
    return pl.pallas_call(
        functools.partial(
            ring_kernel,
            blocks=blocks,
            halves=halves,
            parties=parties,
            arrivals=-1 if own else len(received),
            ordered=after is not None,
        ),
        grid_spec=pltpu.PrefetchScalarGridSpec(
            num_scalar_prefetch=1,
            grid=(1,),
            in_specs=in_specs,
            out_specs=out_specs,
            scratch_shapes=[
                pltpu.VMEM((8, td, h), bf16),
                pltpu.VMEM((rows, h), f32),
                pltpu.SemaphoreType.DMA((8,)),
            ]
            + extra,
        ),
        out_shape=out_shape,
        compiler_params=pltpu.CompilerParams(vmem_limit_bytes=36 * 2**20),
        cost_estimate=pl.CostEstimate(
            flops=4 * depth * width * rows // parties + 4 * 10**9,
            bytes_accessed=2 * depth * width // parties,
            transcendentals=0,
        ),
        name=f"ring_{rows}",
    )(z, *args)


def settle_kernel(picks, own, *refs):
    refs = list(refs)
    payload, logits, picked = refs[-3:]
    pairs = refs[:-3]
    rows, width = own.shape
    h = width // 2
    nodes, lanes = picked.shape[0], payload.shape[1]
    stat_rows = stat_height(nodes, width)
    per = width // lanes
    seqs = (payload.shape[0] - 2 * stat_rows) // per
    halves = [own[:, 0:h], own[:, h:width]]
    for group in range(len(pairs) // 2):
        forward, backward = decode(pairs[2 * group]), decode(pairs[2 * group + 1])
        if group == 0:
            halves = [halves[0] + forward, halves[1] + backward]
        else:
            halves = [halves[0] + backward, halves[1] + forward]
    top = jnp.maximum(*[jnp.max(half, axis=1, keepdims=True) for half in halves])
    total = jnp.zeros((rows, 1), f32)
    for i, half in enumerate(halves):
        logits[:, i * h : (i + 1) * h] = half
        total = total + jnp.sum(jnp.exp(half - top), axis=1, keepdims=True)
    lse = top + jnp.log(total)
    for n in range(seqs):
        for j in range(per):
            payload[n * per + j : n * per + j + 1, :] = logits[n : n + 1, j * lanes : (j + 1) * lanes]
    flat = iota((8, 128), 0) * 128 + iota((8, 128), 1)
    sub = iota((8, 128), 0)
    picked[...] = jnp.zeros(picked.shape, f32)

    def pick(i, carry):
        base = pl.multiple_of(jnp.minimum(picks[0, i], rows - 8), 8)
        start = pl.multiple_of(picks[1, i], 128)
        tile = logits[pl.ds(base, 8), pl.ds(start, 128)]
        value = jnp.sum(jnp.where(flat == picks[2, i], tile, 0.0), axis=0, keepdims=True)
        node = picks[3, i]
        block = pl.ds(pl.multiple_of(node // 8 * 8, 8), 8)
        picked[block, :] = jnp.where(sub == node % 8, value, picked[block, :])
        return carry

    lax.fori_loop(0, picks[4, 0], pick, 0)
    target = jnp.sum(picked[...], axis=1, keepdims=True)
    for i in range(stat_rows):
        match = iota((rows, lanes), 0) == iota((rows, lanes), 1) + i * lanes
        at = seqs * per + i
        payload[at : at + 1, :] = to_row(match, lse)
        match = iota((nodes, lanes), 0) == iota((nodes, lanes), 1) + i * lanes
        at = seqs * per + stat_rows + i
        payload[at : at + 1, :] = to_row(match, target)


def stat_height(nodes, width):
    return pl.cdiv(nodes, width)


def settle(picks, own, pairs, seqs):
    rows, width = own.shape
    nodes = picks.shape[1]
    lanes = min(width, nodes)
    height = seqs * (width // lanes) + 2 * stat_height(nodes, width)
    return pl.pallas_call(
        settle_kernel,
        grid_spec=pltpu.PrefetchScalarGridSpec(
            num_scalar_prefetch=1,
            grid=(1,),
            in_specs=[whole(a.shape) for a in (own, *pairs)],
            out_specs=whole((height, lanes)),
            scratch_shapes=[pltpu.VMEM((rows, width), f32), pltpu.VMEM((nodes, 128), f32)],
        ),
        out_shape=jax.ShapeDtypeStruct((height, lanes), f32),
        compiler_params=pltpu.CompilerParams(vmem_limit_bytes=36 * 2**20),
        name=f"settle_{rows}",
    )(picks, own, *pairs)


def combine_kernel(*refs):
    stats = refs[-1]
    parts = refs[:-1]
    nodes, lanes = stats.shape[1], parts[0].shape[1]
    stat_rows = nodes // lanes
    head = parts[0].shape[0] - 2 * stat_rows
    for i in range(stat_rows):
        values = [ref[head + i : head + i + 1, :] for ref in parts]
        top = functools.reduce(jnp.maximum, values)
        total = sum(jnp.exp(value - top) for value in values)
        stats[0:1, i * lanes : (i + 1) * lanes] = top + jnp.log(total)
        at = head + stat_rows + i
        stats[1:2, i * lanes : (i + 1) * lanes] = sum(ref[at : at + 1, :] for ref in parts)


def combine(payloads, nodes):
    return pl.pallas_call(
        combine_kernel,
        grid=(1,),
        in_specs=[whole(a.shape) for a in payloads],
        out_specs=whole((2, nodes)),
        out_shape=jax.ShapeDtypeStruct((2, nodes), f32),
        compiler_params=pltpu.CompilerParams(vmem_limit_bytes=16 * 2**20),
        name="combine",
    )(*payloads)


def finish_kernel(place, counts, stats, *refs, parties, seqs):
    refs = list(refs)
    leaves = [refs.pop(0) for _ in range(parties)]
    prow, parent, prob, uniform, reach, vertex, lineage, score = refs
    nodes = prow.shape[1]
    tree = nodes // seqs
    out_rows = vertex.shape[1]
    top = jnp.max(stats[:, 0, :], axis=0, keepdims=True)
    total = jnp.sum(jnp.exp(stats[:, 0, :] - top), axis=0, keepdims=True)
    target = jnp.sum(stats[:, 1, :], axis=0, keepdims=True)
    square = (nodes, nodes)
    up, side = iota(square, 0), iota(square, 1)
    log_total = to_col(up == side, top + jnp.log(total))
    width = score.shape[1] // parties
    lanes = leaves[0].shape[1]
    per = width // lanes
    for j, ref in enumerate(leaves):
        start = (place[1] + parties - j) % parties * width
        for k in range(per):
            rows = jnp.concatenate([ref[n * per + k : n * per + k + 1, :] for n in range(seqs)], axis=0)
            column = pl.multiple_of(start + k * lanes, lanes)
            score[:, pl.ds(column, lanes)] = rows - log_total[0:seqs, :]
    margin = target - to_row(up == prow[...], log_total) - jnp.log(prob[...]) - jnp.log(uniform[...])
    index = iota((1, nodes), 1)
    root = parent[...] == index
    live = index < 0
    for s in range(seqs):
        inside = (index >= s * tree) & (index < (s + 1) * tree)
        live = live | (inside & (index - s * tree < counts[s]))
    keep = jnp.logical_not(root) & live
    bounded = jnp.where(root, big_margin, margin)
    path = jnp.min(jnp.where(reach[...].astype(f32) > 0, bounded, big_margin), axis=1, keepdims=True)
    kept = to_col(up == side, jnp.where(keep, 1.0, 0.0))
    vertex_col = to_col(up == side, jnp.where(keep, margin, 0.0))
    local = iota((nodes, out_rows), 0) == iota((nodes, out_rows), 1) + place[0] * out_rows
    vertex[...] = to_row(local, vertex_col)
    lineage[...] = to_row(local, jnp.where(kept > 0, path, 0.0))


def finish(place, counts, stats, leaves, prow, parent, prob, uniform, reach, out_rows, width):
    parties = len(leaves)
    nodes = prow.shape[1]
    seqs = counts.shape[0]
    smem = pl.BlockSpec(memory_space=pltpu.SMEM)
    rows = [prow, parent.reshape(1, nodes), prob.reshape(1, nodes), uniform.reshape(1, nodes)]
    arrays = [stats, *leaves, *rows, reach]
    return pl.pallas_call(
        functools.partial(finish_kernel, parties=parties, seqs=seqs),
        grid=(1,),
        in_specs=[smem, smem] + [whole(a.shape) for a in arrays],
        out_specs=[whole((1, out_rows)), whole((1, out_rows)), whole((seqs, width))],
        out_shape=[
            jax.ShapeDtypeStruct((1, out_rows), f32),
            jax.ShapeDtypeStruct((1, out_rows), f32),
            jax.ShapeDtypeStruct((seqs, width), f32),
        ],
        compiler_params=pltpu.CompilerParams(vmem_limit_bytes=36 * 2**20),
        name="finish",
    )(place, counts, *arrays)


def gathered(hidden, marker):
    size = lax.axis_size("gx")
    if size != 8:
        return [lax.all_gather(hidden, "gx", axis=0, tiled=True)]

    def swap(value, k):
        return lax.ppermute(value, "gx", [(i, i ^ k) for i in range(size)])

    parts = [None] * size
    parts[0] = hidden
    parts[1] = swap(hidden, 1)
    for k in (6, 2, 4):
        parts[k] = swap(hidden, k)
    for k in (2, 4, 6):
        passed, marker = lax.optimization_barrier((parts[k], marker))
        parts[k + 1] = swap(passed, 1)
    return parts


def bucket_sizes(nodes, h):
    sizes = []
    for k in (5, 6, 7, 8, 9, 10):
        sizes.append(nodes * k // 16)
    largest = nodes
    while largest - pl.cdiv(largest, lanes_for(largest, h)) < nodes:
        largest += 16
    return sizes + [largest]


def local(hidden, lm_head, parent, draft_token, draft_prob, uniforms, node_count, accepted_end):
    nodes = parent.shape[0]
    seqs = node_count.shape[0]
    out_rows = hidden.shape[0]
    parties = lax.axis_size("gy")
    h = lm_head.shape[1] // parties // 2
    gx, gy = lax.axis_index("gx").astype(i32), lax.axis_index("gy").astype(i32)
    place = jnp.concatenate([gx.reshape(1), gy.reshape(1)])
    sizes = bucket_sizes(nodes, h)
    sel, reach, prow, picks, branch = prep(
        place,
        node_count,
        accepted_end,
        parent,
        draft_token,
        seqs,
        out_rows,
        lax.axis_size("gx") == 8,
        sizes[-1],
        [size - pl.cdiv(size, lanes_for(size, h)) for size in sizes[:-1]],
        (lm_head.shape[1], lm_head.shape[1] // parties),
    )
    parts = gathered(hidden, branch)
    z = gy.reshape(1)

    def shift(value, k):
        return lax.ppermute(value, "gy", [(i, (i + k) % parties) for i in range(parties)])

    def run(rows):
        def body():
            state = {"lhs": (sel, parts), "after": None}

            def product(halves, received, own=False):
                out = ring_product(
                    z, state["lhs"], lm_head, rows, halves, parties, received, own, state["after"]
                )
                if isinstance(state["lhs"], tuple):
                    state["lhs"], out = out[0], out[1:]
                state["after"] = out[0]
                return out

            def exchange(out):
                return [shift(out[0], 1), shift(out[1], -1)]

            reach_out = parties // 2
            major = exchange(product(((reach_out, 0), (-reach_out, 1)), []))
            minor = []
            for d in range(reach_out - 1, 0, -1):
                minor = exchange(product(((d, 1), (-d, 0)), minor))
                major = exchange(product(((d, 0), (-d, 1)), major))
            own = product(((0, 0), (0, 1)), [], own=True)
            return settle(picks, own[0], [*major, *minor], seqs)

        return body

    payload = lax.switch(branch[0, 0], [run(size) for size in sizes])
    payloads = [payload] + [shift(payload, k) for k in range(1, parties)]
    stats = lax.all_gather(combine(payloads, nodes), "gx")
    vertex, lineage, score = finish(
        place,
        node_count,
        stats,
        payloads,
        prow,
        parent,
        draft_prob,
        uniforms,
        reach,
        out_rows,
        lm_head.shape[1],
    )
    return vertex.reshape(out_rows), lineage.reshape(out_rows), score


def solution(mesh):
    return jax.shard_map(
        local,
        mesh=mesh,
        in_specs=(P("gx", "gy"), P("gy", "gx"), P(), P(), P(), P(), P(), P()),
        out_specs=(P("gx"), P("gx"), P(None, "gx")),
        check_vma=False,
    )
```

```python
import functools

import jax
import jax.numpy as jnp
from jax import lax
from jax.experimental import pallas as pl
from jax.experimental.pallas import tpu as pltpu
from jax.sharding import PartitionSpec as P


big_margin = 10000.0
f32 = jnp.float32
bf16 = jnp.bfloat16
i32 = jnp.int32
i16 = jnp.int16
STEPS = 256.0
LEVELS = 32760.0
VMEM_LIMIT = 56 * 1024 * 1024


def iota(shape, dim):
    return lax.broadcasted_iota(i32, shape, dim)


def to_row(mask, col):
    return jnp.sum(jnp.where(mask, col, 0.0), axis=0, keepdims=True)


def to_col(mask, row):
    return jnp.sum(jnp.where(mask, row, 0.0), axis=1, keepdims=True)


def whole(shape):
    return pl.BlockSpec(shape, lambda *_: (0,) * len(shape))


def prep_kernel(place, counts, ends, parent_row, token, sel, reach, prow, picks, branch, *, seqs, block, xor, limits, spans):
    nodes = parent_row.shape[1]
    tree = nodes // seqs
    square = (nodes, nodes)
    up, side = iota(square, 0), iota(square, 1)
    prow_in = parent_row[...]
    pcol_in = to_col(up == side, prow_in.astype(f32)).astype(i32)

    def flags(index, parents):
        live = index < 0
        end = jnp.full(index.shape, -1, i32)
        for s in range(seqs):
            inside = (index >= s * tree) & (index < (s + 1) * tree)
            live = live | (inside & (index - s * tree < counts[s]))
            end = jnp.where(index == s * tree + ends[s], s, end)
        want = jnp.where(live & (parents != index), 1.0, 0.0).astype(f32)
        return want, end

    row_i, col_i = iota((1, nodes), 1), iota((nodes, 1), 0)
    want_row, end_row = flags(row_i, prow_in)
    want_col, end_col = flags(col_i, pcol_in)
    need_col = jnp.max(jnp.where(prow_in == up, want_row, 0.0), axis=1, keepdims=True)
    need_row = jnp.max(jnp.where(pcol_in == side, want_col, 0.0), axis=0, keepdims=True)
    other_col = jnp.where(end_col >= 0, 0.0, need_col)
    other_row = jnp.where(end_row >= 0, 0.0, need_row)
    before = to_col(side < up, other_row) + seqs
    pos_col = jnp.where(end_col >= 0, end_col.astype(f32), jnp.where(other_col > 0, before, -1.0))
    parent_pos = to_row(up == prow_in, pos_col).astype(i32)
    prow[...] = parent_pos
    total = jnp.sum(other_row, axis=1, keepdims=True) + seqs
    choice = jnp.zeros((1, 1), f32)
    for limit in limits:
        choice = choice + jnp.where(total > limit, 1.0, 0.0)
    branch[...] = jnp.broadcast_to(choice, branch.shape).astype(i32)
    width, quarter = spans
    column = token[...] - (place[0] * width + place[1] * quarter)
    inside = (column >= 0) & (column < quarter) & (parent_pos >= 0)
    safe = jnp.clip(column, 0, quarter - 1)
    row = jnp.maximum(parent_pos, 0)
    hit = jnp.where(inside, 1.0, 0.0)
    rank_col = jnp.where(to_col(up == side, hit) > 0, to_col(side < up, hit), -1.0)
    chosen = rank_col == side.astype(f32)
    fields = [row // 8 * 8, safe // 128 * 128, row % 8 * 128 + safe % 128, row_i]
    for i, field in enumerate(fields):
        picks[i : i + 1, :] = to_row(chosen, to_col(up == side, field.astype(f32))).astype(i32)
    found = jnp.sum(hit, axis=1, keepdims=True)
    picks[4:5, :] = jnp.broadcast_to(found, (1, nodes)).astype(i32)
    if xor:
        origin = (lax.bitwise_xor(row_i // block, place[0])) * block + row_i % block
    else:
        origin = row_i
    pos_x = to_row(up == origin, pos_col)
    sel[...] = jnp.where(pos_x == iota(sel.shape, 0).astype(f32), 1.0, 0.0).astype(bf16)
    chain = jnp.where((pcol_in == side) | (up == side), 1.0, 0.0).astype(bf16)
    for _ in range((tree - 1).bit_length()):
        chain = jnp.minimum(jnp.dot(chain, chain, preferred_element_type=f32), 1.0).astype(bf16)
    reach[...] = chain


def prep(place, counts, ends, parent, token, seqs, block, xor, padded, limits, spans):
    nodes = parent.shape[0]
    smem = pl.BlockSpec(memory_space=pltpu.SMEM)
    return pl.pallas_call(
        functools.partial(
            prep_kernel, seqs=seqs, block=block, xor=xor, limits=limits, spans=spans
        ),
        in_specs=[smem, smem, smem, whole((1, nodes)), whole((1, nodes))],
        out_specs=[whole((padded, nodes)), whole((nodes, nodes)), whole((1, nodes)), whole((5, nodes)), whole((1, 128))],
        out_shape=[
            jax.ShapeDtypeStruct((padded, nodes), bf16),
            jax.ShapeDtypeStruct((nodes, nodes), bf16),
            jax.ShapeDtypeStruct((1, nodes), i32),
            jax.ShapeDtypeStruct((5, nodes), i32),
            jax.ShapeDtypeStruct((1, 128), i32),
        ],
        grid=(1,),
        compiler_params=pltpu.CompilerParams(vmem_limit_bytes=VMEM_LIMIT),
        cost_estimate=pl.CostEstimate(flops=4 * 10**9, bytes_accessed=4 * nodes * nodes, transcendentals=0),
        name="prep",
    )(place, counts, ends, parent.reshape(1, nodes), token.reshape(1, nodes))


def lanes_for(rows, width):
    return min(width, pl.cdiv(rows, 128) * 128)


def encode(value, out):
    rows, width = value.shape
    top = jnp.maximum(jnp.max(jnp.abs(value), axis=1, keepdims=True), 1e-20)
    code = jnp.ceil(jnp.log(top) * (STEPS / jnp.log(2.0).astype(f32)))
    inverse = LEVELS * jnp.exp2(code * (-1.0 / STEPS))
    coded = jnp.round(value * inverse)
    out[...] = coded.astype(i32).astype(i16)
    lanes = lanes_for(rows, width)
    spare = pl.cdiv(rows, lanes)
    tail = coded[rows - 16 : rows, 0:lanes]
    slot = iota((16, 1), 0)
    for i in range(spare):
        match = iota((rows, lanes), 0) == iota((rows, lanes), 1) + i * lanes
        tail = jnp.where(slot == 16 - spare + i, to_row(match, code), tail)
    out[rows - 16 : rows, 0:lanes] = tail.astype(i32).astype(i16)


def decode(ref):
    rows, width = ref.shape
    lanes = lanes_for(rows, width)
    spare = pl.cdiv(rows, lanes)
    tail = ref[rows - 16 : rows, 0:lanes].astype(i32).astype(f32)
    code = jnp.zeros((rows, 1), f32)
    for i in range(spare):
        match = iota((rows, lanes), 0) == iota((rows, lanes), 1) + i * lanes
        code = code + to_col(match, tail[16 - spare + i : 17 - spare + i, :])
    scale = jnp.exp2(code * (1.0 / STEPS)) * (1.0 / LEVELS)
    return ref[...].astype(i32).astype(f32) * scale


def tile_fetch(z, weights, buffer, ready, halves, parties):
    tiles, td, h = buffer.shape
    quarter = weights.shape[1] // parties
    per = tiles // 2
    starts = [
        lax.rem(z[0] + parties + distance, parties) * quarter + side * h for distance, side in halves
    ]

    def fetch(tile):
        column = pl.multiple_of(jnp.where(tile < per, starts[0], starts[1]), h)
        depth = pl.multiple_of(lax.rem(tile, per) * td, td)
        return pltpu.make_async_copy(
            weights.at[pl.ds(depth, td), pl.ds(column, h)], buffer.at[tile], ready.at[tile]
        )

    return fetch


def ahead_kernel(z, weights, marker, buffer, passed, ready, *, halves, parties):
    fetch = tile_fetch(z, weights, buffer, ready, halves, parties)
    tiles = buffer.shape[0]
    for tile in range(tiles):
        fetch(tile).start()
    passed[...] = marker[...]
    for tile in range(tiles):
        fetch(tile).wait()


def read_ahead(z, weights, marker, halves, parties):
    depth, width = weights.shape
    shape = (8, depth // 4, width // parties // 2)
    return pl.pallas_call(
        functools.partial(ahead_kernel, halves=halves, parties=parties),
        grid_spec=pltpu.PrefetchScalarGridSpec(
            num_scalar_prefetch=1,
            grid=(1,),
            in_specs=[pl.BlockSpec(memory_space=pl.ANY), whole(marker.shape)],
            out_specs=[pl.BlockSpec(memory_space=pltpu.VMEM), whole(marker.shape)],
            scratch_shapes=[pltpu.SemaphoreType.DMA((8,))],
        ),
        out_shape=[
            pltpu.VMEM(shape, bf16),
            jax.ShapeDtypeStruct(marker.shape, marker.dtype),
        ],
        compiler_params=pltpu.CompilerParams(vmem_limit_bytes=26 * 2**20),
        cost_estimate=pl.CostEstimate(flops=4 * 10**9, bytes_accessed=16 * 2**20, transcendentals=0),
        name="read_ahead",
    )(z, weights, marker)


def ring_kernel(z, *refs, blocks, halves, parties, arrivals, ordered):
    refs = list(refs)
    first, own = blocks > 0, arrivals < 0
    if first:
        sel = refs.pop(0)
        parts = [refs.pop(0) for _ in range(blocks)]
        buffer = refs.pop(0)
    else:
        lhs = refs.pop(0)
        weights = refs.pop(0)
    received = [refs.pop(0) for _ in range(max(arrivals, 0))]
    if ordered:
        refs.pop(0)
    if first:
        lhs = refs.pop(0)
    outs = [refs.pop(0) for _ in range(1 if own else 2)]
    if first:
        acc, stacked = refs
    else:
        acc, buffer, ready = refs
        fetch = tile_fetch(z, weights, buffer, ready, halves, parties)
        for tile in range(buffer.shape[0]):
            fetch(tile).start()
    tiles, td, h = buffer.shape
    per = tiles // 2
    if first:
        height = parts[0].shape[0]
        for j, part in enumerate(parts):
            stacked[j * height : (j + 1) * height, :] = part[...]
        span = min(512, stacked.shape[1])

        def compact(j, carry):
            column = pl.ds(pl.multiple_of(j * span, span), span)
            lhs[:, column] = jnp.dot(
                sel[...], stacked[:, column], preferred_element_type=f32
            ).astype(bf16)
            return carry

        lax.fori_loop(0, stacked.shape[1] // span, compact, 0)

    def finish_half(i):
        if own:
            outs[0][:, i * h : (i + 1) * h] = acc[...]
            return
        value = acc[...]
        if arrivals:
            value = value + decode(received[i])
        encode(value, outs[i])

    def step(tile, carry):
        if not first:
            fetch(tile).wait()
        j = lax.rem(tile, per)
        depth = pl.multiple_of(j * td, td)
        value = jnp.dot(lhs[:, pl.ds(depth, td)], buffer[tile], preferred_element_type=f32)
        acc[...] = value + jnp.where(j == 0, 0.0, acc[...])
        for i in range(2):
            pl.when(tile == (i + 1) * per - 1)(functools.partial(finish_half, i))
        return carry

    acc[...] = jnp.zeros(acc.shape, f32)
    lax.fori_loop(0, tiles, step, 0)


def ring_product(z, lhs, weights, rows, halves, parties, received, own, after):
    depth, width = weights.shape
    h = width // parties // 2
    td = depth // 4
    anywhere = pl.BlockSpec(memory_space=pl.ANY)
    out_shape, out_specs, extra = [], [], []
    first = isinstance(lhs, tuple)
    blocks = 0
    if first:
        sel, parts, early = lhs
        nodes = sel.shape[1]
        blocks = len(parts)
        args = [sel, *parts, early]
        in_specs = [whole((rows, nodes))] + [whole(part.shape) for part in (*parts, early)]
        out_shape.append(jax.ShapeDtypeStruct((rows, depth), bf16))
        out_specs.append(whole((rows, depth)))
        extra.append(pltpu.VMEM((nodes, depth), bf16))
    else:
        args, in_specs = [lhs, weights], [whole((rows, depth)), anywhere]
        extra += [pltpu.VMEM((8, td, h), bf16), pltpu.SemaphoreType.DMA((8,))]
    args.extend(received)
    in_specs.extend(whole(a.shape) for a in received)
    if after is not None:
        args.append(after)
        in_specs.append(anywhere)
    if own:
        out_shape.append(jax.ShapeDtypeStruct((rows, 2 * h), f32))
        out_specs.append(whole((rows, 2 * h)))
    else:
        out_shape.extend([jax.ShapeDtypeStruct((rows, h), i16)] * 2)
        out_specs.extend([whole((rows, h))] * 2)
    return pl.pallas_call(
        functools.partial(
            ring_kernel,
            blocks=blocks,
            halves=halves,
            parties=parties,
            arrivals=-1 if own else len(received),
            ordered=after is not None,
        ),
        grid_spec=pltpu.PrefetchScalarGridSpec(
            num_scalar_prefetch=1,
            grid=(1,),
            in_specs=in_specs,
            out_specs=out_specs,
            scratch_shapes=[pltpu.VMEM((rows, h), f32)] + extra,
        ),
        out_shape=out_shape,
        compiler_params=pltpu.CompilerParams(vmem_limit_bytes=26 * 2**20),
        cost_estimate=pl.CostEstimate(
            flops=4 * depth * width * rows // parties + 4 * 10**9,
            bytes_accessed=2 * depth * width // parties,
            transcendentals=0,
        ),
        name=f"ring_{rows}",
    )(z, *args)


def settle_kernel(picks, own, *refs):
    refs = list(refs)
    payload, logits, picked = refs[-3:]
    pairs = refs[:-3]
    rows, width = own.shape
    h = width // 2
    nodes, lanes = picked.shape[0], payload.shape[1]
    stat_rows = stat_height(nodes, width)
    per = width // lanes
    seqs = (payload.shape[0] - 2 * stat_rows) // per
    halves = [own[:, 0:h], own[:, h:width]]
    for group in range(len(pairs) // 2):
        forward, backward = decode(pairs[2 * group]), decode(pairs[2 * group + 1])
        if group == 0:
            halves = [halves[0] + forward, halves[1] + backward]
        else:
            halves = [halves[0] + backward, halves[1] + forward]
    top = jnp.maximum(*[jnp.max(half, axis=1, keepdims=True) for half in halves])
    total = jnp.zeros((rows, 1), f32)
    for i, half in enumerate(halves):
        logits[:, i * h : (i + 1) * h] = half
        total = total + jnp.sum(jnp.exp(half - top), axis=1, keepdims=True)
    lse = top + jnp.log(total)
    for n in range(seqs):
        for j in range(per):
            payload[n * per + j : n * per + j + 1, :] = logits[n : n + 1, j * lanes : (j + 1) * lanes]
    flat = iota((8, 128), 0) * 128 + iota((8, 128), 1)
    sub = iota((8, 128), 0)
    picked[...] = jnp.zeros(picked.shape, f32)

    def pick(i, carry):
        base = pl.multiple_of(jnp.minimum(picks[0, i], rows - 8), 8)
        start = pl.multiple_of(picks[1, i], 128)
        tile = logits[pl.ds(base, 8), pl.ds(start, 128)]
        value = jnp.sum(jnp.where(flat == picks[2, i], tile, 0.0), axis=0, keepdims=True)
        node = picks[3, i]
        block = pl.ds(pl.multiple_of(node // 8 * 8, 8), 8)
        picked[block, :] = jnp.where(sub == node % 8, value, picked[block, :])
        return carry

    lax.fori_loop(0, picks[4, 0], pick, 0)
    target = jnp.sum(picked[...], axis=1, keepdims=True)
    for i in range(stat_rows):
        match = iota((rows, lanes), 0) == iota((rows, lanes), 1) + i * lanes
        at = seqs * per + i
        payload[at : at + 1, :] = to_row(match, lse)
        match = iota((nodes, lanes), 0) == iota((nodes, lanes), 1) + i * lanes
        at = seqs * per + stat_rows + i
        payload[at : at + 1, :] = to_row(match, target)


def stat_height(nodes, width):
    return pl.cdiv(nodes, width)


def settle(picks, own, pairs, seqs):
    rows, width = own.shape
    nodes = picks.shape[1]
    lanes = min(width, nodes)
    height = seqs * (width // lanes) + 2 * stat_height(nodes, width)
    return pl.pallas_call(
        settle_kernel,
        grid_spec=pltpu.PrefetchScalarGridSpec(
            num_scalar_prefetch=1,
            grid=(1,),
            in_specs=[whole(a.shape) for a in (own, *pairs)],
            out_specs=whole((height, lanes)),
            scratch_shapes=[pltpu.VMEM((rows, width), f32), pltpu.VMEM((nodes, 128), f32)],
        ),
        out_shape=jax.ShapeDtypeStruct((height, lanes), f32),
        compiler_params=pltpu.CompilerParams(vmem_limit_bytes=26 * 2**20),
        name=f"settle_{rows}",
    )(picks, own, *pairs)


def combine_kernel(*refs):
    stats = refs[-1]
    parts = refs[:-1]
    nodes, lanes = stats.shape[1], parts[0].shape[1]
    stat_rows = nodes // lanes
    head = parts[0].shape[0] - 2 * stat_rows
    for i in range(stat_rows):
        values = [ref[head + i : head + i + 1, :] for ref in parts]
        top = functools.reduce(jnp.maximum, values)
        total = sum(jnp.exp(value - top) for value in values)
        stats[0:1, i * lanes : (i + 1) * lanes] = top + jnp.log(total)
        at = head + stat_rows + i
        stats[1:2, i * lanes : (i + 1) * lanes] = sum(ref[at : at + 1, :] for ref in parts)


def combine(payloads, nodes):
    return pl.pallas_call(
        combine_kernel,
        grid=(1,),
        in_specs=[whole(a.shape) for a in payloads],
        out_specs=whole((2, nodes)),
        out_shape=jax.ShapeDtypeStruct((2, nodes), f32),
        compiler_params=pltpu.CompilerParams(vmem_limit_bytes=16 * 2**20),
        name="combine",
    )(*payloads)


def finish_kernel(place, counts, stats, *refs, parties, seqs):
    refs = list(refs)
    leaves = [refs.pop(0) for _ in range(parties)]
    prow, parent, prob, uniform, reach, vertex, lineage, score = refs
    nodes = prow.shape[1]
    tree = nodes // seqs
    out_rows = vertex.shape[1]
    top = jnp.max(stats[:, 0, :], axis=0, keepdims=True)
    total = jnp.sum(jnp.exp(stats[:, 0, :] - top), axis=0, keepdims=True)
    target = jnp.sum(stats[:, 1, :], axis=0, keepdims=True)
    square = (nodes, nodes)
    up, side = iota(square, 0), iota(square, 1)
    log_total = to_col(up == side, top + jnp.log(total))
    width = score.shape[1] // parties
    lanes = leaves[0].shape[1]
    per = width // lanes
    for j, ref in enumerate(leaves):
        start = (place[1] + parties - j) % parties * width
        for k in range(per):
            rows = jnp.concatenate([ref[n * per + k : n * per + k + 1, :] for n in range(seqs)], axis=0)
            column = pl.multiple_of(start + k * lanes, lanes)
            score[:, pl.ds(column, lanes)] = rows - log_total[0:seqs, :]
    margin = target - to_row(up == prow[...], log_total) - jnp.log(prob[...]) - jnp.log(uniform[...])
    index = iota((1, nodes), 1)
    root = parent[...] == index
    live = index < 0
    for s in range(seqs):
        inside = (index >= s * tree) & (index < (s + 1) * tree)
        live = live | (inside & (index - s * tree < counts[s]))
    keep = jnp.logical_not(root) & live
    bounded = jnp.where(root, big_margin, margin)
    path = jnp.min(jnp.where(reach[...].astype(f32) > 0, bounded, big_margin), axis=1, keepdims=True)
    kept = to_col(up == side, jnp.where(keep, 1.0, 0.0))
    vertex_col = to_col(up == side, jnp.where(keep, margin, 0.0))
    local = iota((nodes, out_rows), 0) == iota((nodes, out_rows), 1) + place[0] * out_rows
    vertex[...] = to_row(local, vertex_col)
    lineage[...] = to_row(local, jnp.where(kept > 0, path, 0.0))


def finish(place, counts, stats, leaves, prow, parent, prob, uniform, reach, out_rows, width):
    parties = len(leaves)
    nodes = prow.shape[1]
    seqs = counts.shape[0]
    smem = pl.BlockSpec(memory_space=pltpu.SMEM)
    rows = [prow, parent.reshape(1, nodes), prob.reshape(1, nodes), uniform.reshape(1, nodes)]
    arrays = [stats, *leaves, *rows, reach]
    return pl.pallas_call(
        functools.partial(finish_kernel, parties=parties, seqs=seqs),
        grid=(1,),
        in_specs=[smem, smem] + [whole(a.shape) for a in arrays],
        out_specs=[whole((1, out_rows)), whole((1, out_rows)), whole((seqs, width))],
        out_shape=[
            jax.ShapeDtypeStruct((1, out_rows), f32),
            jax.ShapeDtypeStruct((1, out_rows), f32),
            jax.ShapeDtypeStruct((seqs, width), f32),
        ],
        compiler_params=pltpu.CompilerParams(vmem_limit_bytes=26 * 2**20),
        name="finish",
    )(place, counts, *arrays)


def gathered(hidden, marker):
    size = lax.axis_size("gx")
    if size != 8:
        return [lax.all_gather(hidden, "gx", axis=0, tiled=True)]

    def swap(value, k):
        return lax.ppermute(value, "gx", [(i, i ^ k) for i in range(size)])

    parts = [None] * size
    parts[0] = hidden
    parts[1] = swap(hidden, 1)
    for k in (6, 2, 4):
        parts[k] = swap(hidden, k)
    for k in (2, 4, 6):
        passed, marker = lax.optimization_barrier((parts[k], marker))
        parts[k + 1] = swap(passed, 1)
    return parts


def bucket_sizes(nodes, h):
    sizes = []
    for k in (5, 6, 7, 8, 9, 10):
        sizes.append(nodes * k // 16)
    largest = nodes
    while largest - pl.cdiv(largest, lanes_for(largest, h)) < nodes:
        largest += 16
    return sizes + [largest]


def local(hidden, lm_head, parent, draft_token, draft_prob, uniforms, node_count, accepted_end):
    nodes = parent.shape[0]
    seqs = node_count.shape[0]
    out_rows = hidden.shape[0]
    parties = lax.axis_size("gy")
    h = lm_head.shape[1] // parties // 2
    gx, gy = lax.axis_index("gx").astype(i32), lax.axis_index("gy").astype(i32)
    place = jnp.concatenate([gx.reshape(1), gy.reshape(1)])
    sizes = bucket_sizes(nodes, h)
    sel, reach, prow, picks, branch = prep(
        place,
        node_count,
        accepted_end,
        parent,
        draft_token,
        seqs,
        out_rows,
        lax.axis_size("gx") == 8,
        sizes[-1],
        [size - pl.cdiv(size, lanes_for(size, h)) for size in sizes[:-1]],
        (lm_head.shape[1], lm_head.shape[1] // parties),
    )
    z = gy.reshape(1)
    farthest = ((parties // 2, 0), (-(parties // 2), 1))
    early, branch = read_ahead(z, lm_head, branch, farthest, parties)
    parts = gathered(hidden, branch)
    def shift(value, k):
        return lax.ppermute(value, "gy", [(i, (i + k) % parties) for i in range(parties)])

    def run(rows):
        def body():
            state = {"lhs": (sel, parts, early), "after": None}

            def product(halves, received, own=False):
                out = ring_product(
                    z, state["lhs"], lm_head, rows, halves, parties, received, own, state["after"]
                )
                if isinstance(state["lhs"], tuple):
                    state["lhs"], out = out[0], out[1:]
                state["after"] = out[0]
                return out

            def exchange(out):
                return [shift(out[0], 1), shift(out[1], -1)]

            reach_out = parties // 2
            major = exchange(product(farthest, []))
            minor = []
            for d in range(reach_out - 1, 0, -1):
                minor = exchange(product(((d, 1), (-d, 0)), minor))
                major = exchange(product(((d, 0), (-d, 1)), major))
            own = product(((0, 0), (0, 1)), [], own=True)
            return settle(picks, own[0], [*major, *minor], seqs)

        return body

    payload = lax.switch(branch[0, 0], [run(size) for size in sizes])
    payloads = [payload] + [shift(payload, k) for k in range(1, parties)]
    stats = lax.all_gather(combine(payloads, nodes), "gx")
    vertex, lineage, score = finish(
        place,
        node_count,
        stats,
        payloads,
        prow,
        parent,
        draft_prob,
        uniforms,
        reach,
        out_rows,
        lm_head.shape[1],
    )
    return vertex.reshape(out_rows), lineage.reshape(out_rows), score


def solution(mesh):
    return jax.shard_map(
        local,
        mesh=mesh,
        in_specs=(P("gx", "gy"), P("gy", "gx"), P(), P(), P(), P(), P(), P()),
        out_specs=(P("gx"), P("gx"), P(None, "gx")),
        check_vma=False,
    )
```
